128 devices in a mesh: owner: 8 (over x, core), server: 16 (over z, y).
Axes of the slice: x: 4, y: 4, z: 4, core: 2. Of those that a mesh axis runs over, the one named last changes fastest.
Arguments:
- queries: bfloat16 [32768, 1024], P(('owner', 'server')), may hold values from -8 to 8
- key_vectors: bfloat16 [32768, 128], P(('owner', 'server')), may hold values from -8 to 8
- value_vectors: bfloat16 [32768, 128], P(('owner', 'server')), may hold values from -6 to 6
- out_grad: bfloat16 [32768, 1024], P(('owner', 'server')), may hold values from -6 to 6
- segments: int32 [32768], replicated, may hold values from 0 to 31, never falling along the last dimension, each value on 1 to 2048 neighbouring positions
- phase_label: int32 [128], P(('owner', 'server')), may hold values 0 or 1
Outputs:
- attn_out: bfloat16 [32768, 1024], P(('owner', 'server'))
- grad_query: bfloat16 [32768, 1024], P(('owner', 'server'))
- grad_key: float32 [32768, 128], P(('owner', 'server'))
- grad_value: float32 [32768, 128], P(('owner', 'server'))
The draws below stay inside these ranges and needn't reach their ends.
All inputs are finite; a program needn't handle non-finite values. No bound on the sum of `phase_label` on one device may be relied on, other than what follows from the above.
Results may differ from the reference program's by a relative error of at most 0.012.
The reference program's roundings to bfloat16 on the way (of `weights` and `grad_score`) count: a program that leaves them out, or rounds other values in their place, can miss the bound.
Values may be sent and summed in bfloat16 or wider, within the bound.
A program may use at most 128 MiB of HBM per device.

```python
import math
import jax
import jax.numpy as jnp
import numpy as np
from jax import lax

HEAD = 128
QHEADS = 8
TOK_DEV = 256
REACH = 8
TOKENS = 32768
DEVICES = 128


def draw_key_vectors(key, part):
    base = jnp.clip(jax.random.normal(jax.random.fold_in(key, 3), (TOKENS, HEAD), jnp.float32), -6.0, 6.0)
    return base.astype(jnp.bfloat16)


def draw_queries(key, part):
    base = jnp.clip(jax.random.normal(jax.random.fold_in(key, 5), (TOKENS, QHEADS * HEAD), jnp.float32), -6.0, 6.0)
    return base.astype(jnp.bfloat16)


def plant(drawn, stream_key, low, high):
    extent = drawn.shape
    spot = [jax.random.randint(jax.random.fold_in(stream_key, axis), (), 0, extent[axis]) for axis in range(len(extent))]
    drawn = drawn.at[tuple(spot)].set(low)
    longest = extent.index(max(extent))
    spot[longest] = (spot[longest] + 1) % extent[longest]
    return drawn.at[tuple(spot)].set(high)


def level_of(stream_key, shape, cuts, smallest, high):
    level = 1.0
    for position, parts in cuts:
        heights = jax.random.uniform(jax.random.fold_in(jax.random.fold_in(stream_key, 6), position), (parts,), jnp.float32, smallest / len(cuts), high / len(cuts))
        level = level * jnp.repeat(jnp.exp(heights), shape[position] // parts).reshape((-1,) + (1,) * (len(shape) - 1 - position))
    return level


def profile(amount, total, bound, lean):
    loads = [(1 << 20) // math.isqrt(grade ** lean) + 1 for grade in range(2, amount + 1)]
    rest, given = total - bound - (amount - 1), [1] * (amount - 1)
    while rest > 0:
        free = [i for i in range(amount - 1) if given[i] < bound]
        mass, left = sum([loads[i] for i in free]), rest
        for i in free:
            more = min(bound - given[i], max(1, left * loads[i] // mass), rest)
            given[i] = given[i] + more
            rest = rest - more
    return np.array([bound] + given)


def uneven_parts(stream_key, count, total, reach, skew):
    if count == 2:
        one = jax.random.randint(stream_key, (), max(1, total - reach), min(reach, total - 1) + 1)
        return jnp.stack([one, total - one])
    sizes = jnp.asarray(profile(count, total, reach, skew), jnp.int32)
    twos = (count - 1) // 2
    donor, receiver = sizes[1:1 + 2 * twos:2], sizes[2:2 + 2 * twos:2]
    room = jnp.minimum(donor - 1, reach - receiver)
    passed = jax.random.randint(jax.random.fold_in(stream_key, 1), (twos,), 0, 1 << 20) % (room + 1)
    sizes = sizes.at[1:1 + 2 * twos:2].set(donor - passed).at[2:2 + 2 * twos:2].set(receiver + passed)
    return sizes[jax.random.permutation(jax.random.fold_in(stream_key, 2), count)]


def noise(stream_key, shape, spread, most, split=(), held_as=jnp.bfloat16):
    drawn = jax.random.normal(stream_key, shape, jnp.float32) * spread
    if len(split) > 0:
        drawn = level_of(stream_key, shape, split, -0.22, 0.18) * drawn
    return jnp.clip(drawn, min=-most, max=most).astype(held_as)


def setup_inputs(seed: int = 0) -> dict:
    key_of = jax.random.split(jax.random.key(seed), 7)
    queries = draw_queries(jax.random.fold_in(key_of[6], 71), 0)
    key_vectors = draw_key_vectors(jax.random.fold_in(key_of[6], 71), 0)
    value_vectors = noise(key_of[2], (TOKENS, HEAD), 1.0, 6.0, ((0, 128),))
    out_grad = noise(key_of[3], (TOKENS, QHEADS * HEAD), 1.0, 6.0, ((0, 128),))
    segments = jnp.searchsorted(jnp.cumsum(uneven_parts(key_of[4], 2 * TOKENS // (REACH * TOK_DEV), TOKENS, REACH * TOK_DEV, 1)), jnp.arange(TOKENS), side="right").astype(jnp.int32)
    phase_label = plant((jax.random.randint(key_of[5], (DEVICES,), 0, 2) < 1).astype(jnp.int32), jax.random.fold_in(key_of[5], 1), 0, 1)
    return {"queries": queries, "key_vectors": key_vectors, "value_vectors": value_vectors, "out_grad": out_grad, "segments": segments, "phase_label": phase_label}


def tile_pass(query_tile, grad_tile, key_window, value_window, allowed, pong_flag):
    score_scale = HEAD ** -0.5
    outputs = []
    query_grads = []
    key_grad = jnp.zeros(key_window.shape, jnp.float32)
    value_grad = jnp.zeros(value_window.shape, jnp.float32)
    for head_index in range(QHEADS):
        query_head = query_tile[:, head_index * HEAD:(head_index + 1) * HEAD]
        grad_head = grad_tile[:, head_index * HEAD:(head_index + 1) * HEAD]
        score = jnp.dot(query_head, key_window.T, preferred_element_type=jnp.float32) * score_scale
        score = jnp.where(allowed, score, -1e30)
        row_top = jnp.max(score, axis=1, keepdims=True)
        expos = jnp.exp(score - row_top)
        row_total = jnp.sum(expos, axis=1, keepdims=True)
        weights = expos.astype(jnp.bfloat16)
        head_out = jnp.dot(weights, value_window, preferred_element_type=jnp.float32) / row_total
        out_rounded = head_out.astype(jnp.bfloat16)
        outputs.append(out_rounded)
        row_delta = jnp.sum(grad_head.astype(jnp.float32) * out_rounded.astype(jnp.float32), axis=1, keepdims=True)
        probs_full = expos / row_total
        grad_prob = jnp.dot(grad_head, value_window.T, preferred_element_type=jnp.float32)
        grad_score = (probs_full * (grad_prob - row_delta) * score_scale).astype(jnp.bfloat16)
        query_grads.append(jnp.dot(grad_score, key_window, preferred_element_type=jnp.float32) * pong_flag)
        key_grad = key_grad + jnp.dot(grad_score.T, query_head, preferred_element_type=jnp.float32) * pong_flag
        value_grad = value_grad + jnp.dot(probs_full.astype(jnp.bfloat16).T, grad_head, preferred_element_type=jnp.float32) * pong_flag
    return jnp.concatenate(outputs, axis=1), jnp.concatenate(query_grads, axis=1).astype(jnp.bfloat16), key_grad, value_grad


def reference(queries, key_vectors, value_vectors, out_grad, segments, phase_label):
    tiles = TOKENS // TOK_DEV
    key_span = (REACH + 1) * TOK_DEV
    pad_rows = REACH * TOK_DEV
    keys_padded = jnp.concatenate([jnp.zeros((pad_rows, HEAD), key_vectors.dtype), key_vectors], axis=0)
    values_padded = jnp.concatenate([jnp.zeros((pad_rows, HEAD), value_vectors.dtype), value_vectors], axis=0)
    segs_padded = jnp.concatenate([jnp.full((pad_rows,), -1, jnp.int32), segments.astype(jnp.int32)], axis=0)
    causal = jnp.arange(key_span)[None, :] <= jnp.arange(TOK_DEV)[:, None] + pad_rows

    def scan_step(carried, tile_index):
        key_total, value_total = carried
        row_start = (tile_index * TOK_DEV).astype(jnp.int32)
        query_tile = lax.dynamic_slice_in_dim(queries, row_start, TOK_DEV, 0)
        grad_tile = lax.dynamic_slice_in_dim(out_grad, row_start, TOK_DEV, 0)
        key_window = lax.dynamic_slice_in_dim(keys_padded, row_start, key_span, 0)
        value_window = lax.dynamic_slice_in_dim(values_padded, row_start, key_span, 0)
        key_segs = lax.dynamic_slice_in_dim(segs_padded, row_start, key_span, 0)
        query_segs = lax.dynamic_slice_in_dim(segments.astype(jnp.int32), row_start, TOK_DEV, 0)
        allowed = causal & (query_segs[:, None] == key_segs[None, :])
        pong_flag = lax.dynamic_slice_in_dim(phase_label, tile_index, 1, 0).astype(jnp.float32)[0]
        tile_out, tile_dq, key_grad, value_grad = tile_pass(query_tile, grad_tile, key_window, value_window, allowed, pong_flag)
        old_key = lax.dynamic_slice_in_dim(key_total, row_start, key_span, 0)
        old_value = lax.dynamic_slice_in_dim(value_total, row_start, key_span, 0)
        key_total = lax.dynamic_update_slice_in_dim(key_total, old_key + key_grad, row_start, 0)
        value_total = lax.dynamic_update_slice_in_dim(value_total, old_value + value_grad, row_start, 0)
        return (key_total, value_total), (tile_out, tile_dq)

    initial = (jnp.zeros((TOKENS + pad_rows, HEAD), jnp.float32), jnp.zeros((TOKENS + pad_rows, HEAD), jnp.float32))
    totals, stacked = lax.scan(scan_step, initial, jnp.arange(tiles, dtype=jnp.int32))
    attn_out = stacked[0].reshape(TOKENS, QHEADS * HEAD)
    grad_query = stacked[1].reshape(TOKENS, QHEADS * HEAD)
    return attn_out, grad_query, totals[0][pad_rows:], totals[1][pad_rows:]
```

```python
import functools
import math

import jax
import jax.numpy as jnp
from jax import lax
from jax.experimental import pallas as pl
from jax.experimental.pallas import tpu as pltpu
from jax.sharding import PartitionSpec as P

MESH = pl.DeviceIdType.MESH
REACH = 8
SLOTS = REACH + 1
ROW = 4
FAR = -1e30
UNROLL_F = 2
UNROLL_B = 2
F32 = jnp.float32
BF16 = jnp.bfloat16


def fused(
    heads, scale, servers, tiles,
    q_hbm, k_hbm, v_hbm, do_hbm, seg_ref, phase_ref,
    o_ref, dq_ref, dk_ref, dv_ref,
    q_s, do_s, qt_s, dot_s, win, win_t, s_s, dp_s, bias_s, m_s, l_s, d_s, ot_s, dqt_s,
    acc, out_buf, in_buf,
    load_sem, fsend, frecv, bsend, brecv,
):
    tok, width = q_s.shape[1], q_s.shape[2]
    owner = lax.axis_index("owner")
    server = lax.axis_index("server")
    tile = owner * servers + server
    y = server % ROW
    first, last = (y + 3) // 4, y // 3

    def at_tile(t):
        t = (t + tiles) % tiles
        return (t // servers, t % servers)

    up, down = at_tile(tile + ROW), at_tile(tile - ROW)
    row_start = server - y
    right = (owner, row_start + (y + 1) % ROW)
    left = (owner, row_start + (y + 3) % ROW)

    loads = [pltpu.make_async_copy(k_hbm, win.at[0, 0], load_sem.at[0]),
             pltpu.make_async_copy(v_hbm, win.at[0, 1], load_sem.at[1])]
    for h in range(heads):
        cols = pl.ds(h * width, width)
        loads.append(pltpu.make_async_copy(q_hbm.at[:, cols], q_s.at[h], load_sem.at[2 + h]))
        loads.append(pltpu.make_async_copy(do_hbm.at[:, cols], do_s.at[h], load_sem.at[2 + heads + h]))
    for copy in loads:
        copy.start()

    barrier = pltpu.get_barrier_semaphore()
    for peer in (up, down, left, right):
        pl.semaphore_signal(barrier, inc=1, device_id=peer, device_id_type=MESH)
    pl.semaphore_wait(barrier, 4)

    def block(src, dst, send, half, peer):
        return pltpu.make_async_remote_copy(
            src_ref=win.at[src, half], dst_ref=win.at[dst, half],
            send_sem=fsend.at[send, half], recv_sem=frecv.at[dst, half],
            device_id=peer, device_id_type=MESH)

    def send_block(src, dst, send, peer):
        for half in range(2):
            block(src, dst, send, half, peer).start()

    def wait_block(slot):
        for half in range(2):
            block(slot, slot, 0, half, left).wait_recv()

    loads[0].wait()
    loads[1].wait()
    send_block(0, 4, 0, up)

    @pl.when(y != 3)
    def _():
        send_block(0, 1, 1, right)

    @pl.when(y == 0)
    def _():
        send_block(0, 3, 2, left)

    for copy in loads[2:]:
        copy.wait()
    for h in range(heads):
        qt_s[h] = q_s[h].T
        dot_s[h] = do_s[h].T

    log2e = 1.4426950408889634
    q_seg = seg_ref[pl.ds(tile, 1), :]

    def forward(slot):
        owner_tile = tile - slot
        k_seg = seg_ref[pl.ds((owner_tile + tiles) % tiles, 1), :]
        k_seg = jnp.where(owner_tile >= 0, k_seg, -1)
        k_col = jnp.broadcast_to(k_seg.astype(F32), (128, tok)).T
        k_col = jnp.concatenate([k_col] * (tok // 128), axis=1)
        seen = k_col == q_seg.astype(F32)
        if slot == 0:
            key_at = lax.broadcasted_iota(jnp.int32, (tok, tok), 0)
            query_at = lax.broadcasted_iota(jnp.int32, (tok, tok), 1)
            seen = seen & (key_at <= query_at)
        bias_s[...] = jnp.where(seen, 0.0, FAR)
        win_t[slot, 0] = win[slot, 0].T
        win_t[slot, 1] = win[slot, 1].T

        def some_heads(step, carry):
            for part in range(UNROLL_F):
                h = step * UNROLL_F + part
                s = jnp.dot(win[slot, 0], qt_s[h], preferred_element_type=F32)
                s = s * (scale * log2e) + bias_s[...]
                s_s[slot, h] = s
                top = jnp.max(s, axis=0, keepdims=True)
                if slot == 0:
                    p = jnp.exp2(s - top)
                    l_s[h] = jnp.sum(p, axis=0, keepdims=True)
                    ot_s[h] = jnp.dot(win_t[slot, 1], p.astype(BF16), preferred_element_type=F32)
                    m_s[h] = top
                else:
                    old = m_s[h]
                    top = jnp.maximum(old, top)
                    shrink = jnp.exp2(old - top)
                    p = jnp.exp2(s - top)
                    l_s[h] = l_s[h] * shrink + jnp.sum(p, axis=0, keepdims=True)
                    ot_s[h] = ot_s[h] * shrink + jnp.dot(
                        win_t[slot, 1], p.astype(BF16), preferred_element_type=F32)
                    m_s[h] = top
                dp_s[slot, h] = jnp.dot(win[slot, 1], dot_s[h], preferred_element_type=F32)
            return carry

        lax.fori_loop(0, heads // UNROLL_F, some_heads, 0)

    forward(0)

    wait_block(4)
    send_block(4, 8, 3, up)

    @pl.when(y == 3)
    def _():
        send_block(4, 1, 1, right)

    @pl.when(y != 0)
    def _():
        send_block(4, 3, 2, left)

    @pl.when(y != 3)
    def _():
        send_block(4, 5, 4, right)

    @pl.when(y == 0)
    def _():
        send_block(4, 7, 5, left)

    forward(4)

    wait_block(1)

    @pl.when(y != 3)
    def _():
        send_block(1, 2, 6, right)

    forward(1)

    wait_block(8)

    @pl.when(y == 3)
    def _():
        send_block(8, 5, 4, right)

    @pl.when(y != 0)
    def _():
        send_block(8, 7, 5, left)

    wait_block(3)

    @pl.when(y == 0)
    def _():
        send_block(3, 6, 7, left)

    forward(3)
    wait_block(5)

    @pl.when(y == 3)
    def _():
        send_block(5, 2, 6, right)

    forward(8)
    wait_block(7)

    @pl.when(y != 0)
    def _():
        send_block(7, 6, 7, left)

    forward(5)
    forward(7)
    wait_block(2)
    forward(2)
    wait_block(6)
    forward(6)

    def finish_head(h, carry):
        total = l_s[h]
        out_t = (ot_s[h] / total).astype(BF16)
        d_s[h] = jnp.sum(dot_s[h].astype(F32) * out_t.astype(F32), axis=0, keepdims=True)
        m_s[h] = m_s[h] + jnp.log2(total)
        cols = pl.ds(pl.multiple_of(h * width, width), width)
        o_ref[:, cols] = out_t.T
        return carry

    lax.fori_loop(0, heads, finish_head, 0)

    def backward(slot, first_slot=False):
        def some_heads(step, carry):
            key_part = None
            for part in range(UNROLL_B):
                h = step * UNROLL_B + part
                p = jnp.exp2(s_s[slot, h] - m_s[h])
                ds = (p * (dp_s[slot, h] - d_s[h])).astype(BF16)
                pb = p.astype(BF16)
                dq = jnp.dot(win_t[slot, 0], ds, preferred_element_type=F32)
                if first_slot:
                    dqt_s[h] = dq
                else:
                    dqt_s[h] = dqt_s[h] + dq
                dk = jnp.dot(ds, q_s[h], preferred_element_type=F32)
                dv = jnp.dot(pb, do_s[h], preferred_element_type=F32)
                key_part = dk if key_part is None else key_part + dk
                value_part = dv if part == 0 else value_part + dv
            return (carry[0] + key_part, carry[1] + value_part)

        zero = jnp.zeros((tok, width), F32)
        dk, dv = lax.fori_loop(0, heads // UNROLL_B, some_heads, (zero, zero))
        flag = phase_ref[0].astype(F32)
        acc[slot, 0] = dk * (scale * flag)
        acc[slot, 1] = dv * flag

    def part(slot, half, peer):
        return pltpu.make_async_remote_copy(
            src_ref=out_buf.at[slot, half], dst_ref=in_buf.at[slot, half],
            send_sem=bsend.at[slot, half], recv_sem=brecv.at[slot, half],
            device_id=peer, device_id_type=MESH)

    def send_half(slot, half, peer):
        out_buf[slot, half] = acc[slot, half].astype(BF16)
        part(slot, half, peer).start()

    def send_part(slot, peer):
        for half in range(2):
            send_half(slot, half, peer)

    def take_half(slot, into, half):
        part(slot, half, left).wait_recv()
        acc[into, half] = acc[into, half] + in_buf[slot, half].astype(F32)

    backward(2, True)
    send_part(2, left)
    backward(6)
    send_part(6, right)
    backward(1)
    backward(5)
    send_part(5 - 4 * last, left)
    backward(3)
    backward(7)
    send_part(7 - 4 * first, right)
    for half in range(2):
        take_half(2, 1 + 4 * last, half)
        send_half(1 + 4 * last, half, left)
        take_half(6, 3 + 4 * first, half)
        send_half(3 + 4 * first, half, right)
    backward(8)
    backward(4)
    backward(0)

    def finish_query(h, carry):
        flag = phase_ref[0].astype(F32)
        cols = pl.ds(pl.multiple_of(h * width, width), width)
        dq_ref[:, cols] = (dqt_s[h] * (scale * flag)).astype(BF16).T
        return carry

    lax.fori_loop(0, heads, finish_query, 0)

    for half in range(2):
        take_half(5, 4 + 4 * last, half)
        take_half(7, 4 + 4 * first, half)
        take_half(1, 4 * last, half)
        take_half(3, 4 * first, half)
        send_half(8, half, down)
    for half in range(2):
        take_half(8, 4, half)
        send_half(4, half, down)
    for half in range(2):
        take_half(4, 0, half)
    dk_ref[...] = acc[0, 0]
    dv_ref[...] = acc[0, 1]

    for half in range(2):
        for send in range(8):
            block(0, 0, send, half, left).wait_send()
        for slot in range(1, SLOTS):
            part(slot, half, left).wait_send()


def solution(mesh):
    servers = mesh.shape["server"]
    tiles = servers * mesh.shape["owner"]

    def on_device(queries, key_vectors, value_vectors, out_grad, segments, phase_label):
        tok, width = key_vectors.shape
        heads = queries.shape[1] // width
        seg_rows = segments.reshape(tiles, tok)
        vmem = pl.BlockSpec(memory_space=pltpu.VMEM)
        anywhere = pl.BlockSpec(memory_space=pl.ANY)
        smem = pl.BlockSpec(memory_space=pltpu.SMEM)
        return pl.pallas_call(
            functools.partial(fused, heads, 1.0 / math.sqrt(width), servers, tiles),
            out_shape=(
                jax.ShapeDtypeStruct((tok, heads * width), BF16),
                jax.ShapeDtypeStruct((tok, heads * width), BF16),
                jax.ShapeDtypeStruct((tok, width), F32),
                jax.ShapeDtypeStruct((tok, width), F32),
            ),
            in_specs=[anywhere, anywhere, anywhere, anywhere, vmem, smem],
            out_specs=(vmem, vmem, vmem, vmem),
            scratch_shapes=[
                pltpu.VMEM((heads, tok, width), BF16),
                pltpu.VMEM((heads, tok, width), BF16),
                pltpu.VMEM((heads, width, tok), BF16),
                pltpu.VMEM((heads, width, tok), BF16),
                pltpu.VMEM((SLOTS, 2, tok, width), BF16),
                pltpu.VMEM((SLOTS, 2, width, tok), BF16),
                pltpu.VMEM((SLOTS, heads, tok, tok), F32),
                pltpu.VMEM((SLOTS, heads, tok, tok), F32),
                pltpu.VMEM((tok, tok), F32),
                pltpu.VMEM((heads, 1, tok), F32),
                pltpu.VMEM((heads, 1, tok), F32),
                pltpu.VMEM((heads, 1, tok), F32),
                pltpu.VMEM((heads, width, tok), F32),
                pltpu.VMEM((heads, width, tok), F32),
                pltpu.VMEM((SLOTS, 2, tok, width), F32),
                pltpu.VMEM((SLOTS, 2, tok, width), BF16),
                pltpu.VMEM((SLOTS, 2, tok, width), BF16),
                pltpu.SemaphoreType.DMA((2 + 2 * heads,)),
                pltpu.SemaphoreType.DMA((8, 2)),
                pltpu.SemaphoreType.DMA((SLOTS, 2)),
                pltpu.SemaphoreType.DMA((SLOTS, 2)),
                pltpu.SemaphoreType.DMA((SLOTS, 2)),
            ],
            compiler_params=pltpu.CompilerParams(
                collective_id=0, has_side_effects=True, vmem_limit_bytes=60 * 1024 * 1024
            ),
        )(queries, key_vectors, value_vectors, out_grad, seg_rows, phase_label)

    tokens = P(("owner", "server"), None)
    return jax.shard_map(
        on_device,
        mesh=mesh,
        in_specs=(tokens, tokens, tokens, tokens, P(), P(("owner", "server"))),
        out_specs=(tokens, tokens, tokens, tokens),
        check_vma=False,
    )
```

```python
import functools
import math

import jax
import jax.numpy as jnp
from jax import lax
from jax.experimental import pallas as pl
from jax.experimental.pallas import tpu as pltpu
from jax.sharding import PartitionSpec as P

MESH = pl.DeviceIdType.MESH
REACH = 8
SLOTS = REACH + 1
ROW = 4
FAR = -1e30
LAG = 3
CUTS = 2
F32 = jnp.float32
BF16 = jnp.bfloat16


def fused(
    heads, scale, servers, tiles,
    q_hbm, k_hbm, v_hbm, do_hbm, seg_hbm, phase_ref,
    o_ref, dq_ref, dk_ref, dv_ref,
    q_s, do_s, qt_s, dot_s, win, win_t, seg_s, s_s, dp_s, bias_s, m_s, l_s, d_s, ot_s, outt_s, dqt_s,
    acc, out_buf, in_buf,
    load_sem, fsend, frecv, bsend, brecv,
):
    tok, width = q_s.shape[1], q_s.shape[2]
    owner = lax.axis_index("owner")
    server = lax.axis_index("server")
    tile = owner * servers + server
    y = server % ROW
    first, last = (y + 3) // 4, y // 3
    rows_of = [pl.ds(k * (tok // CUTS), tok // CUTS) for k in range(CUTS)]
    pieces = [(half, cut) for half in range(2) for cut in range(CUTS)]

    def at_tile(t):
        t = (t + tiles) % tiles
        return (t // servers, t % servers)

    up, down = at_tile(tile + ROW), at_tile(tile - ROW)
    row_start = server - y
    right = (owner, row_start + (y + 1) % ROW)
    left = (owner, row_start + (y + 3) % ROW)

    loads = [pltpu.make_async_copy(k_hbm, win.at[0, 0], load_sem.at[0]),
             pltpu.make_async_copy(v_hbm, win.at[0, 1], load_sem.at[1]),
             pltpu.make_async_copy(seg_hbm, seg_s, load_sem.at[2])]
    for h in range(heads):
        cols = pl.ds(h * width, width)
        loads.append(pltpu.make_async_copy(q_hbm.at[:, cols], q_s.at[h], load_sem.at[3 + h]))
        loads.append(pltpu.make_async_copy(do_hbm.at[:, cols], do_s.at[h], load_sem.at[3 + heads + h]))
    for copy in loads:
        copy.start()

    barrier = pltpu.get_barrier_semaphore()
    for peer in (up, down, left, right):
        pl.semaphore_signal(barrier, inc=1, device_id=peer, device_id_type=MESH)
    pl.semaphore_wait(barrier, 4)

    def block(src, dst, send, half, cut, peer):
        return pltpu.make_async_remote_copy(
            src_ref=win.at[src, half, rows_of[cut]], dst_ref=win.at[dst, half, rows_of[cut]],
            send_sem=fsend.at[send, half, cut], recv_sem=frecv.at[dst, half, cut],
            device_id=peer, device_id_type=MESH)

    def pass_on(slot, *moves):
        for half, cut in pieces:
            if slot:
                block(slot, slot, 0, half, cut, left).wait_recv()
            elif cut == 0:
                loads[half].wait()
            for when, dst, send, peer in moves:
                if when is None:
                    block(slot, dst, send, half, cut, peer).start()
                else:
                    @pl.when(when)
                    def _():
                        block(slot, dst, send, half, cut, peer).start()

    pass_on(0, (None, 4, 0, up), (y != 3, 1, 1, right), (y == 0, 3, 2, left))

    for copy in loads[2:]:
        copy.wait()
    for h in range(heads):
        qt_s[h] = q_s[h].T
        dot_s[h] = do_s[h].T

    log2e = 1.4426950408889634
    seg_rows = tok // 128

    def seg_row(t):
        parts = [seg_s[pl.ds(t * seg_rows + k, 1), :] for k in range(seg_rows)]
        return jnp.concatenate(parts, axis=1)

    q_seg = seg_row(tile).astype(F32)

    def eight_rows(x, op):
        total = x[0:8]
        for k in range(1, x.shape[0] // 8):
            total = op(total, x[k * 8:(k + 1) * 8])
        return total

    def forward(slot):
        owner_tile = tile - slot
        k_seg = seg_row((owner_tile + tiles) % tiles)
        k_seg = jnp.where(owner_tile >= 0, k_seg, -1)
        k_col = jnp.broadcast_to(k_seg.astype(F32), (128, tok)).T
        k_col = jnp.concatenate([k_col] * (tok // 128), axis=1)
        seen = k_col == q_seg
        if slot == 0:
            key_at = lax.broadcasted_iota(jnp.int32, (tok, tok), 0)
            query_at = lax.broadcasted_iota(jnp.int32, (tok, tok), 1)
            seen = seen & (key_at <= query_at)
        bias_s[...] = jnp.where(seen, 0.0, FAR)
        win_t[slot, 0] = win[slot, 0].T
        win_t[slot, 1] = win[slot, 1].T

        def scores(h):
            s = jnp.dot(win[slot, 0], qt_s[h], preferred_element_type=F32)
            s = s * (scale * log2e) + bias_s[...]
            s_s[slot, h] = s
            dp_s[slot, h] = jnp.dot(win[slot, 1], dot_s[h], preferred_element_type=F32)
            return jnp.max(eight_rows(s, jnp.maximum), axis=0, keepdims=True)

        def weigh(h, top):
            if slot:
                old = m_s[h]
                top = jnp.maximum(old, top)
                shrink = jnp.exp2(old - top)
            p = jnp.exp2(s_s[slot, h] - top)
            total = jnp.sum(eight_rows(p, jnp.add), axis=0, keepdims=True)
            out_t = jnp.dot(win_t[slot, 1], p.astype(BF16), preferred_element_type=F32)
            m_s[h] = top
            l_s[h] = l_s[h] * shrink + total if slot else total
            ot_s[h] = ot_s[h] * shrink + out_t if slot else out_t

        tops = []
        for h in range(heads + LAG):
            if h < heads:
                tops.append(scores(h))
            if h >= LAG:
                weigh(h - LAG, tops[h - LAG])

    forward(0)
    pass_on(4, (None, 8, 3, up), (y != 0, 3, 2, left), (y == 0, 7, 5, left), (y == 3, 1, 1, right), (y != 3, 5, 4, right))
    pass_on(1, (y != 3, 2, 6, right))
    forward(4)
    pass_on(8, (y != 0, 7, 5, left), (y == 3, 5, 4, right))
    pass_on(3, (y == 0, 6, 7, left))
    forward(1)
    pass_on(5, (y == 3, 2, 6, right))
    pass_on(7, (y != 0, 6, 7, left))
    forward(3)
    forward(8)
    forward(5)
    forward(7)
    pass_on(2)
    forward(2)
    pass_on(6)
    forward(6)

    for h in range(heads):
        total = l_s[h]
        out_t = (ot_s[h] * (1.0 / total)).astype(BF16)
        outt_s[h] = out_t
        d_s[h] = jnp.sum(eight_rows(dot_s[h].astype(F32) * out_t.astype(F32), jnp.add), axis=0, keepdims=True)
        m_s[h] = m_s[h] + jnp.log2(total)

    flag = phase_ref[0].astype(F32)

    def backward(slot, first_slot=False):
        dk = dv = None
        for h in range(heads):
            p = jnp.exp2(s_s[slot, h] - m_s[h])
            ds = (p * (dp_s[slot, h] - d_s[h])).astype(BF16)
            dq = jnp.dot(win_t[slot, 0], ds, preferred_element_type=F32)
            dqt_s[h] = dq if first_slot else dqt_s[h] + dq
            dk_h = jnp.dot(ds, q_s[h], preferred_element_type=F32)
            dv_h = jnp.dot(p.astype(BF16), do_s[h], preferred_element_type=F32)
            dk = dk_h if h == 0 else dk + dk_h
            dv = dv_h if h == 0 else dv + dv_h
        dk, dv = dk * (scale * flag), dv * flag
        acc[slot, 0] = acc[slot, 0] + dk if slot == 4 else dk
        acc[slot, 1] = acc[slot, 1] + dv if slot == 4 else dv

    def part(slot, half, cut, peer):
        return pltpu.make_async_remote_copy(
            src_ref=out_buf.at[slot, half, rows_of[cut]], dst_ref=in_buf.at[slot, half, rows_of[cut]],
            send_sem=bsend.at[slot, half, cut], recv_sem=brecv.at[slot, half, cut],
            device_id=peer, device_id_type=MESH)

    def send_piece(slot, half, cut, peer, when=None):
        def send():
            out_buf[slot, half, rows_of[cut]] = acc[slot, half, rows_of[cut]].astype(BF16)
            part(slot, half, cut, peer).start()

        send() if when is None else pl.when(when)(send)

    def send_part(slot, peer, when=None):
        for half, cut in pieces:
            send_piece(slot, half, cut, peer, when)

    def take_piece(slot, into, half, cut):
        part(slot, half, cut, left).wait_recv()
        rows = rows_of[cut]
        acc[into, half, rows] = acc[into, half, rows] + in_buf[slot, half, rows].astype(F32)

    acc[4] = jnp.zeros(acc.shape[1:], F32)
    backward(6, True)
    send_part(6, right)
    backward(2)
    send_part(2, left)
    backward(7)
    send_part(7, right, y == 0)
    backward(5)
    send_part(5, left, y != 3)
    backward(3)
    for half, cut in pieces:
        take_piece(6, 3 + 4 * first, half, cut)
        send_piece(7, half, cut, right, y != 0)
    send_part(3, right)
    backward(1)
    for half, cut in pieces:
        take_piece(2, 1 + 4 * last, half, cut)
        send_piece(5, half, cut, left, y == 3)
    send_part(1, left)
    backward(8)
    for half, cut in pieces:
        take_piece(7, 4 + 4 * first, half, cut)
        take_piece(5, 4 + 4 * last, half, cut)
        send_piece(8, half, cut, down)
    backward(4)
    backward(0)

    for h in range(heads):
        cols = pl.ds(h * width, width)
        o_ref[:, cols] = outt_s[h].T
        dq_ref[:, cols] = (dqt_s[h] * (scale * flag)).astype(BF16).T

    for half, cut in pieces:
        take_piece(3, 4 * first, half, cut)
        take_piece(1, 4 * last, half, cut)
        take_piece(8, 4, half, cut)
        send_piece(4, half, cut, down)
    for half, cut in pieces:
        take_piece(4, 0, half, cut)
    dk_ref[...] = acc[0, 0]
    dv_ref[...] = acc[0, 1]

    for half, cut in pieces:
        for send in range(8):
            block(0, 0, send, half, cut, left).wait_send()
        for slot in range(1, SLOTS):
            part(slot, half, cut, left).wait_send()


def solution(mesh):
    servers = mesh.shape["server"]
    tiles = servers * mesh.shape["owner"]

    def on_device(queries, key_vectors, value_vectors, out_grad, segments, phase_label):
        tok, width = key_vectors.shape
        heads = queries.shape[1] // width
        seg_rows = segments.reshape(-1, 128)
        vmem = pl.BlockSpec(memory_space=pltpu.VMEM)
        anywhere = pl.BlockSpec(memory_space=pl.ANY)
        smem = pl.BlockSpec(memory_space=pltpu.SMEM)
        return pl.pallas_call(
            functools.partial(fused, heads, 1.0 / math.sqrt(width), servers, tiles),
            out_shape=(
                jax.ShapeDtypeStruct((tok, heads * width), BF16),
                jax.ShapeDtypeStruct((tok, heads * width), BF16),
                jax.ShapeDtypeStruct((tok, width), F32),
                jax.ShapeDtypeStruct((tok, width), F32),
            ),
            in_specs=[anywhere] * 5 + [smem],
            out_specs=(vmem, vmem, vmem, vmem),
            scratch_shapes=[
                pltpu.VMEM((heads, tok, width), BF16),
                pltpu.VMEM((heads, tok, width), BF16),
                pltpu.VMEM((heads, width, tok), BF16),
                pltpu.VMEM((heads, width, tok), BF16),
                pltpu.VMEM((SLOTS, 2, tok, width), BF16),
                pltpu.VMEM((SLOTS, 2, width, tok), BF16),
                pltpu.VMEM((tiles * tok // 128, 128), jnp.int32),
                pltpu.VMEM((SLOTS, heads, tok, tok), F32),
                pltpu.VMEM((SLOTS, heads, tok, tok), F32),
                pltpu.VMEM((tok, tok), F32),
                pltpu.VMEM((heads, 1, tok), F32),
                pltpu.VMEM((heads, 1, tok), F32),
                pltpu.VMEM((heads, 1, tok), F32),
                pltpu.VMEM((heads, width, tok), F32),
                pltpu.VMEM((heads, width, tok), BF16),
                pltpu.VMEM((heads, width, tok), F32),
                pltpu.VMEM((SLOTS, 2, tok, width), F32),
                pltpu.VMEM((SLOTS, 2, tok, width), BF16),
                pltpu.VMEM((SLOTS, 2, tok, width), BF16),
                pltpu.SemaphoreType.DMA((3 + 2 * heads,)),
                pltpu.SemaphoreType.DMA((8, 2, CUTS)),
                pltpu.SemaphoreType.DMA((SLOTS, 2, CUTS)),
                pltpu.SemaphoreType.DMA((SLOTS, 2, CUTS)),
                pltpu.SemaphoreType.DMA((SLOTS, 2, CUTS)),
            ],
            compiler_params=pltpu.CompilerParams(
                collective_id=0, has_side_effects=True, vmem_limit_bytes=60 * 1024 * 1024
            ),
        )(queries, key_vectors, value_vectors, out_grad, seg_rows, phase_label)

    tokens = P(("owner", "server"), None)
    return jax.shard_map(
        on_device,
        mesh=mesh,
        in_specs=(tokens, tokens, tokens, tokens, P(), P(("owner", "server"))),
        out_specs=(tokens, tokens, tokens, tokens),
        check_vma=False,
    )
```

```python
import functools
import math

import jax
import jax.numpy as jnp
from jax import lax
from jax.experimental import pallas as pl
from jax.experimental.pallas import tpu as pltpu
from jax.sharding import PartitionSpec as P

MESH = pl.DeviceIdType.MESH
REACH = 8
SLOTS = REACH + 1
ROW = 4
FAR = -1e30
LAG = 3
CUTS = 2
F32 = jnp.float32
BF16 = jnp.bfloat16


def fused(
    heads, scale, servers, tiles,
    q_hbm, k_hbm, v_hbm, do_hbm, seg_hbm, phase_ref,
    o_ref, dq_ref, dk_ref, dv_ref,
    q_s, do_s, qt_s, dot_s, win, win_t, seg_s, s_s, dp_s, bias_s, m_s, l_s, d_s, ot_s, outt_s, dqt_s,
    acc, out_buf, in_buf,
    load_sem, fsend, frecv, bsend, brecv,
):
    tok, width = q_s.shape[1], q_s.shape[2]
    owner = lax.axis_index("owner")
    server = lax.axis_index("server")
    tile = owner * servers + server
    y = server % ROW
    first, last = (y + 3) // 4, y // 3
    rows_of = [pl.ds(k * (tok // CUTS), tok // CUTS) for k in range(CUTS)]
    pieces = [(half, cut) for half in range(2) for cut in range(CUTS)]

    def at_tile(t):
        t = (t + tiles) % tiles
        return (t // servers, t % servers)

    up, down = at_tile(tile + ROW), at_tile(tile - ROW)
    row_start = server - y
    right = (owner, row_start + (y + 1) % ROW)
    left = (owner, row_start + (y + 3) % ROW)

    loads = [pltpu.make_async_copy(k_hbm, win.at[0, 0], load_sem.at[0]),
             pltpu.make_async_copy(v_hbm, win.at[0, 1], load_sem.at[1]),
             pltpu.make_async_copy(seg_hbm, seg_s, load_sem.at[2])]
    for h in range(heads):
        cols = pl.ds(h * width, width)
        loads.append(pltpu.make_async_copy(q_hbm.at[:, cols], q_s.at[h], load_sem.at[3 + h]))
        loads.append(pltpu.make_async_copy(do_hbm.at[:, cols], do_s.at[h], load_sem.at[3 + heads + h]))
    for copy in loads:
        copy.start()

    barrier = pltpu.get_barrier_semaphore()
    for peer in (up, down, left, right):
        pl.semaphore_signal(barrier, inc=1, device_id=peer, device_id_type=MESH)
    pl.semaphore_wait(barrier, 4)

    def block(src, dst, send, half, cut, peer):
        return pltpu.make_async_remote_copy(
            src_ref=win.at[src, half, rows_of[cut]], dst_ref=win.at[dst, half, rows_of[cut]],
            send_sem=fsend.at[send, half, cut], recv_sem=frecv.at[dst, half, cut],
            device_id=peer, device_id_type=MESH)

    def pass_on(slot, *moves, between=()):
        between = list(between)
        for half, cut in pieces:
            if slot:
                block(slot, slot, 0, half, cut, left).wait_recv()
            elif cut == 0:
                loads[half].wait()
            for when, dst, send, peer in moves:
                if when is None:
                    block(slot, dst, send, half, cut, peer).start()
                else:
                    @pl.when(when)
                    def _():
                        block(slot, dst, send, half, cut, peer).start()
            if between:
                forward(between.pop(0))

    pass_on(0, (None, 4, 0, up), (y != 3, 1, 1, right), (y == 0, 3, 2, left))

    for copy in loads[2:]:
        copy.wait()
    for h in range(heads):
        qt_s[h] = q_s[h].T
        dot_s[h] = do_s[h].T

    log2e = 1.4426950408889634
    seg_rows = tok // 128

    def seg_row(t):
        parts = [seg_s[pl.ds(t * seg_rows + k, 1), :] for k in range(seg_rows)]
        return jnp.concatenate(parts, axis=1)

    q_seg = seg_row(tile).astype(F32)

    def eight_rows(x, op):
        total = x[0:8]
        for k in range(1, x.shape[0] // 8):
            total = op(total, x[k * 8:(k + 1) * 8])
        return total

    def forward(slot):
        owner_tile = tile - slot
        k_seg = seg_row((owner_tile + tiles) % tiles)
        k_seg = jnp.where(owner_tile >= 0, k_seg, -1)
        k_col = jnp.broadcast_to(k_seg.astype(F32), (128, tok)).T
        k_col = jnp.concatenate([k_col] * (tok // 128), axis=1)
        seen = k_col == q_seg
        if slot == 0:
            key_at = lax.broadcasted_iota(jnp.int32, (tok, tok), 0)
            query_at = lax.broadcasted_iota(jnp.int32, (tok, tok), 1)
            seen = seen & (key_at <= query_at)
        bias_s[...] = jnp.where(seen, 0.0, FAR)
        win_t[slot, 0] = win[slot, 0].T
        win_t[slot, 1] = win[slot, 1].T

        def scores(h):
            s = jnp.dot(win[slot, 0], qt_s[h], preferred_element_type=F32)
            s = s * (scale * log2e) + bias_s[...]
            s_s[slot, h] = s
            dp_s[slot, h] = jnp.dot(win[slot, 1], dot_s[h], preferred_element_type=F32)
            return jnp.max(eight_rows(s, jnp.maximum), axis=0, keepdims=True)

        def weigh(h, top):
            if slot:
                old = m_s[h]
                top = jnp.maximum(old, top)
                shrink = jnp.exp2(old - top)
            p = jnp.exp2(s_s[slot, h] - top)
            total = jnp.sum(eight_rows(p, jnp.add), axis=0, keepdims=True)
            out_t = jnp.dot(win_t[slot, 1], p.astype(BF16), preferred_element_type=F32)
            m_s[h] = top
            l_s[h] = l_s[h] * shrink + total if slot else total
            ot_s[h] = ot_s[h] * shrink + out_t if slot else out_t

        tops = []
        for h in range(heads + LAG):
            if h < heads:
                tops.append(scores(h))
            if h >= LAG:
                weigh(h - LAG, tops[h - LAG])

    forward(0)
    pass_on(4, (None, 8, 3, up), (y != 0, 3, 2, left), (y == 0, 7, 5, left), (y == 3, 1, 1, right), (y != 3, 5, 4, right))
    pass_on(1, (y != 3, 2, 6, right))
    forward(4)
    pass_on(8, (y != 0, 7, 5, left), (y == 3, 5, 4, right))
    pass_on(3, (y == 0, 6, 7, left))
    forward(1)
    pass_on(5, (y == 3, 2, 6, right))
    pass_on(7, (y != 0, 6, 7, left), between=(3, 8, 5))
    forward(7)
    pass_on(2)
    forward(2)
    pass_on(6)
    forward(6)

    for h in range(heads):
        total = l_s[h]
        out_t = (ot_s[h] * (1.0 / total)).astype(BF16)
        outt_s[h] = out_t
        d_s[h] = jnp.sum(eight_rows(dot_s[h].astype(F32) * out_t.astype(F32), jnp.add), axis=0, keepdims=True)
        m_s[h] = m_s[h] + jnp.log2(total)

    flag = phase_ref[0].astype(F32)

    def backward(slot, first_slot=False):
        dk = dv = None
        for h in range(heads):
            p = jnp.exp2(s_s[slot, h] - m_s[h])
            ds = (p * (dp_s[slot, h] - d_s[h])).astype(BF16)
            dq = jnp.dot(win_t[slot, 0], ds, preferred_element_type=F32)
            dqt_s[h] = dq if first_slot else dqt_s[h] + dq
            dk_h = jnp.dot(ds, q_s[h], preferred_element_type=F32)
            dv_h = jnp.dot(p.astype(BF16), do_s[h], preferred_element_type=F32)
            dk = dk_h if h == 0 else dk + dk_h
            dv = dv_h if h == 0 else dv + dv_h
        dk, dv = dk * (scale * flag), dv * flag
        acc[slot, 0] = acc[slot, 0] + dk if slot == 4 else dk
        acc[slot, 1] = acc[slot, 1] + dv if slot == 4 else dv

    def part(slot, half, cut, peer):
        return pltpu.make_async_remote_copy(
            src_ref=out_buf.at[slot, half, rows_of[cut]], dst_ref=in_buf.at[slot, half, rows_of[cut]],
            send_sem=bsend.at[slot, half, cut], recv_sem=brecv.at[slot, half, cut],
            device_id=peer, device_id_type=MESH)

    def send_piece(slot, half, cut, peer, when=None):
        def send():
            out_buf[slot, half, rows_of[cut]] = acc[slot, half, rows_of[cut]].astype(BF16)
            part(slot, half, cut, peer).start()

        send() if when is None else pl.when(when)(send)

    def send_part(slot, peer, when=None):
        for half, cut in pieces:
            send_piece(slot, half, cut, peer, when)

    def take_piece(slot, into, half, cut):
        part(slot, half, cut, left).wait_recv()
        rows = rows_of[cut]
        acc[into, half, rows] = acc[into, half, rows] + in_buf[slot, half, rows].astype(F32)

    acc[4] = jnp.zeros(acc.shape[1:], F32)
    backward(6, True)
    send_part(6, right)
    backward(2)
    send_part(2, left)
    backward(7)
    send_part(7, right, y == 0)
    backward(5)
    send_part(5, left, y != 3)
    backward(3)
    for half, cut in pieces:
        take_piece(6, 3 + 4 * first, half, cut)
        send_piece(7, half, cut, right, y != 0)
    send_part(3, right)
    backward(1)
    for half, cut in pieces:
        take_piece(2, 1 + 4 * last, half, cut)
        send_piece(5, half, cut, left, y == 3)
    send_part(1, left)
    backward(8)
    for half, cut in pieces:
        take_piece(7, 4 + 4 * first, half, cut)
        take_piece(5, 4 + 4 * last, half, cut)
        send_piece(8, half, cut, down)
    backward(4)
    backward(0)

    for h in range(heads):
        cols = pl.ds(h * width, width)
        o_ref[:, cols] = outt_s[h].T
        dq_ref[:, cols] = (dqt_s[h] * (scale * flag)).astype(BF16).T

    for half, cut in pieces:
        take_piece(3, 4 * first, half, cut)
        take_piece(1, 4 * last, half, cut)
        take_piece(8, 4, half, cut)
        send_piece(4, half, cut, down)
    for half, cut in pieces:
        take_piece(4, 0, half, cut)
    dk_ref[...] = acc[0, 0]
    dv_ref[...] = acc[0, 1]

    for half, cut in pieces:
        for send in range(8):
            block(0, 0, send, half, cut, left).wait_send()
        for slot in range(1, SLOTS):
            part(slot, half, cut, left).wait_send()


def write_out(*refs):
    count = len(refs) // 2
    sems = refs[-1]
    copies = [pltpu.make_async_copy(refs[k], refs[count + k], sems.at[k]) for k in range(count)]
    for copy in copies:
        copy.start()
    for copy in copies:
        copy.wait()


def solution(mesh):
    servers = mesh.shape["server"]
    tiles = servers * mesh.shape["owner"]

    def on_device(queries, key_vectors, value_vectors, out_grad, segments, phase_label):
        tok, width = key_vectors.shape
        heads = queries.shape[1] // width
        seg_rows = segments.reshape(-1, 128)
        vmem = pl.BlockSpec(memory_space=pltpu.VMEM)
        anywhere = pl.BlockSpec(memory_space=pl.ANY)
        smem = pl.BlockSpec(memory_space=pltpu.SMEM)
        results = pl.pallas_call(
            functools.partial(fused, heads, 1.0 / math.sqrt(width), servers, tiles),
            out_shape=(
                pltpu.VMEM((tok, heads * width), BF16),
                pltpu.VMEM((tok, heads * width), BF16),
                pltpu.VMEM((tok, width), F32),
                pltpu.VMEM((tok, width), F32),
            ),
            in_specs=[anywhere] * 5 + [smem],
            out_specs=(vmem, vmem, vmem, vmem),
            scratch_shapes=[
                pltpu.VMEM((heads, tok, width), BF16),
                pltpu.VMEM((heads, tok, width), BF16),
                pltpu.VMEM((heads, width, tok), BF16),
                pltpu.VMEM((heads, width, tok), BF16),
                pltpu.VMEM((SLOTS, 2, tok, width), BF16),
                pltpu.VMEM((SLOTS, 2, width, tok), BF16),
                pltpu.VMEM((tiles * tok // 128, 128), jnp.int32),
                pltpu.VMEM((SLOTS, heads, tok, tok), F32),
                pltpu.VMEM((SLOTS, heads, tok, tok), F32),
                pltpu.VMEM((tok, tok), F32),
                pltpu.VMEM((heads, 1, tok), F32),
                pltpu.VMEM((heads, 1, tok), F32),
                pltpu.VMEM((heads, 1, tok), F32),
                pltpu.VMEM((heads, width, tok), F32),
                pltpu.VMEM((heads, width, tok), BF16),
                pltpu.VMEM((heads, width, tok), F32),
                pltpu.VMEM((SLOTS, 2, tok, width), F32),
                pltpu.VMEM((SLOTS, 2, tok, width), BF16),
                pltpu.VMEM((SLOTS, 2, tok, width), BF16),
                pltpu.SemaphoreType.DMA((3 + 2 * heads,)),
                pltpu.SemaphoreType.DMA((8, 2, CUTS)),
                pltpu.SemaphoreType.DMA((SLOTS, 2, CUTS)),
                pltpu.SemaphoreType.DMA((SLOTS, 2, CUTS)),
                pltpu.SemaphoreType.DMA((SLOTS, 2, CUTS)),
            ],
            compiler_params=pltpu.CompilerParams(
                collective_id=0, has_side_effects=True, vmem_limit_bytes=54 * 1024 * 1024
            ),
        )(queries, key_vectors, value_vectors, out_grad, seg_rows, phase_label)
        return pl.pallas_call(
            write_out,
            out_shape=[jax.ShapeDtypeStruct(r.shape, r.dtype) for r in results],
            in_specs=[vmem] * len(results),
            out_specs=[anywhere] * len(results),
            scratch_shapes=[pltpu.SemaphoreType.DMA((len(results),))],
            compiler_params=pltpu.CompilerParams(vmem_limit_bytes=1024 * 1024),
        )(*results)

    tokens = P(("owner", "server"), None)
    return jax.shard_map(
        on_device,
        mesh=mesh,
        in_specs=(tokens, tokens, tokens, tokens, P(), P(("owner", "server"))),
        out_specs=(tokens, tokens, tokens, tokens),
        check_vma=False,
    )
```

```python
import functools
import math

import jax
import jax.numpy as jnp
from jax import lax
from jax.experimental import pallas as pl
from jax.experimental.pallas import tpu as pltpu
from jax.sharding import PartitionSpec as P

MESH = pl.DeviceIdType.MESH
REACH = 8
SLOTS = REACH + 1
ROW = 4
FAR = -1e30
LAG = 3
CUTS = 2
F32 = jnp.float32
BF16 = jnp.bfloat16


def fused(
    heads, scale, servers, tiles,
    q_hbm, k_hbm, v_hbm, do_hbm, seg_hbm, phase_ref,
    o_ref, dq_ref, dk_ref, dv_ref,
    q_s, do_s, qt_s, dot_s, win, win_t, seg_s, s_s, dp_s, bias_s, m_s, l_s, d_s, ot_s, outt_s, dqt_s,
    acc, out_buf, in_buf,
    load_sem, fsend, frecv, bsend, brecv,
):
    tok, width = q_s.shape[1], q_s.shape[2]
    owner = lax.axis_index("owner")
    server = lax.axis_index("server")
    tile = owner * servers + server
    y = server % ROW
    first, last = (y + 3) // 4, y // 3
    rows_of = [pl.ds(k * (tok // CUTS), tok // CUTS) for k in range(CUTS)]
    pieces = [(half, cut) for half in range(2) for cut in range(CUTS)]

    def at_tile(t):
        t = (t + tiles) % tiles
        return (t // servers, t % servers)

    up, down = at_tile(tile + ROW), at_tile(tile - ROW)
    row_start = server - y
    right = (owner, row_start + (y + 1) % ROW)
    left = (owner, row_start + (y + 3) % ROW)

    loads = [pltpu.make_async_copy(k_hbm, win.at[0, 0], load_sem.at[0]),
             pltpu.make_async_copy(v_hbm, win.at[0, 1], load_sem.at[1]),
             pltpu.make_async_copy(seg_hbm, seg_s, load_sem.at[2])]
    for h in range(heads):
        cols = pl.ds(h * width, width)
        loads.append(pltpu.make_async_copy(q_hbm.at[:, cols], q_s.at[h], load_sem.at[3 + h]))
        loads.append(pltpu.make_async_copy(do_hbm.at[:, cols], do_s.at[h], load_sem.at[3 + heads + h]))
    for copy in loads:
        copy.start()

    barrier = pltpu.get_barrier_semaphore()
    for peer in (up, down, left, right):
        pl.semaphore_signal(barrier, inc=1, device_id=peer, device_id_type=MESH)
    pl.semaphore_wait(barrier, 4)

    def block(src, dst, send, half, cut, peer):
        return pltpu.make_async_remote_copy(
            src_ref=win.at[src, half, rows_of[cut]], dst_ref=win.at[dst, half, rows_of[cut]],
            send_sem=fsend.at[send, half, cut], recv_sem=frecv.at[dst, half, cut],
            device_id=peer, device_id_type=MESH)

    def pass_on(slot, *moves, between=()):
        between = list(between)
        for half, cut in pieces:
            if slot:
                block(slot, slot, 0, half, cut, left).wait_recv()
            elif cut == 0:
                loads[half].wait()
            for when, dst, send, peer in moves:
                if when is None:
                    block(slot, dst, send, half, cut, peer).start()
                else:
                    @pl.when(when)
                    def _():
                        block(slot, dst, send, half, cut, peer).start()
            if between:
                forward(between.pop(0))

    pass_on(0, (None, 4, 0, up), (y != 3, 1, 1, right), (y == 0, 3, 2, left))

    for copy in loads[2:]:
        copy.wait()
    for h in range(heads):
        qt_s[h] = q_s[h].T
        dot_s[h] = do_s[h].T

    log2e = 1.4426950408889634
    seg_rows = tok // 128

    def seg_row(t):
        parts = [seg_s[pl.ds(t * seg_rows + k, 1), :] for k in range(seg_rows)]
        return jnp.concatenate(parts, axis=1)

    q_seg = seg_row(tile).astype(F32)

    def eight_rows(x, op):
        total = x[0:8]
        for k in range(1, x.shape[0] // 8):
            total = op(total, x[k * 8:(k + 1) * 8])
        return total

    def forward(slot):
        owner_tile = tile - slot
        k_seg = seg_row((owner_tile + tiles) % tiles)
        k_seg = jnp.where(owner_tile >= 0, k_seg, -1)
        k_col = jnp.broadcast_to(k_seg.astype(F32), (128, tok)).T
        k_col = jnp.concatenate([k_col] * (tok // 128), axis=1)
        seen = k_col == q_seg
        if slot == 0:
            key_at = lax.broadcasted_iota(jnp.int32, (tok, tok), 0)
            query_at = lax.broadcasted_iota(jnp.int32, (tok, tok), 1)
            seen = seen & (key_at <= query_at)
        bias_s[...] = jnp.where(seen, 0.0, FAR)
        win_t[slot, 0] = win[slot, 0].T
        win_t[slot, 1] = win[slot, 1].T

        def scores(h):
            s = jnp.dot(win[slot, 0], qt_s[h], preferred_element_type=F32)
            s = s * (scale * log2e) + bias_s[...]
            s_s[slot, h] = s
            dp_s[slot, h] = jnp.dot(win[slot, 1], dot_s[h], preferred_element_type=F32)
            return jnp.max(eight_rows(s, jnp.maximum), axis=0, keepdims=True)

        def weigh(h, top):
            if slot:
                old = m_s[h]
                top = jnp.maximum(old, top)
                shrink = jnp.exp2(old - top)
            p = jnp.exp2(s_s[slot, h] - top)
            total = jnp.sum(eight_rows(p, jnp.add), axis=0, keepdims=True)
            out_t = jnp.dot(win_t[slot, 1], p.astype(BF16), preferred_element_type=F32)
            m_s[h] = top
            l_s[h] = l_s[h] * shrink + total if slot else total
            ot_s[h] = ot_s[h] * shrink + out_t if slot else out_t

        tops = []
        for h in range(heads + LAG):
            if h < heads:
                tops.append(scores(h))
            if h >= LAG:
                weigh(h - LAG, tops[h - LAG])

    forward(0)
    pass_on(4, (None, 8, 3, up), (y != 0, 3, 2, left), (y == 0, 7, 5, left), (y == 3, 1, 1, right), (y != 3, 5, 4, right))
    pass_on(1, (y != 3, 2, 6, right))
    forward(4)
    pass_on(8, (y != 0, 7, 5, left), (y == 3, 5, 4, right))
    pass_on(3, (y == 0, 6, 7, left))
    forward(1)
    pass_on(5, (y == 3, 2, 6, right))
    pass_on(7, (y != 0, 6, 7, left), between=(3, 8, 5))
    forward(7)
    pass_on(2)
    forward(2)
    pass_on(6)
    forward(6)

    for h in range(heads):
        total = l_s[h]
        out_t = (ot_s[h] * (1.0 / total)).astype(BF16)
        outt_s[h] = out_t
        d_s[h] = jnp.sum(eight_rows(dot_s[h].astype(F32) * out_t.astype(F32), jnp.add), axis=0, keepdims=True)
        m_s[h] = m_s[h] + jnp.log2(total)

    flag = phase_ref[0].astype(F32)

    def backward(slot, first_slot=False):
        dk = dv = None
        for h in range(heads):
            p = jnp.exp2(s_s[slot, h] - m_s[h])
            ds = (p * (dp_s[slot, h] - d_s[h])).astype(BF16)
            dq = jnp.dot(win_t[slot, 0], ds, preferred_element_type=F32)
            dqt_s[h] = dq if first_slot else dqt_s[h] + dq
            dk_h = jnp.dot(ds, q_s[h], preferred_element_type=F32)
            dv_h = jnp.dot(p.astype(BF16), do_s[h], preferred_element_type=F32)
            dk = dk_h if h == 0 else dk + dk_h
            dv = dv_h if h == 0 else dv + dv_h
        dk, dv = dk * (scale * flag), dv * flag
        acc[slot, 0] = acc[slot, 0] + dk if slot == 4 else dk
        acc[slot, 1] = acc[slot, 1] + dv if slot == 4 else dv

    def part(slot, half, cut, peer):
        return pltpu.make_async_remote_copy(
            src_ref=out_buf.at[slot, half, rows_of[cut]], dst_ref=in_buf.at[slot, half, rows_of[cut]],
            send_sem=bsend.at[slot, half, cut], recv_sem=brecv.at[slot, half, cut],
            device_id=peer, device_id_type=MESH)

    def send_piece(slot, half, cut, peer, when=None):
        def send():
            out_buf[slot, half, rows_of[cut]] = acc[slot, half, rows_of[cut]].astype(BF16)
            part(slot, half, cut, peer).start()

        send() if when is None else pl.when(when)(send)

    def send_part(slot, peer, when=None):
        for half, cut in pieces:
            send_piece(slot, half, cut, peer, when)

    def take_piece(slot, into, half, cut, when=None):
        def take():
            part(slot, half, cut, left).wait_recv()
            rows = rows_of[cut]
            acc[into, half, rows] = acc[into, half, rows] + in_buf[slot, half, rows].astype(F32)

        take() if when is None else pl.when(when)(take)

    acc[4] = jnp.zeros(acc.shape[1:], F32)
    backward(6, True)
    send_part(6, right)
    backward(2)
    send_part(2, left)
    backward(7)
    send_part(7, right, y == 0)
    backward(5)
    send_part(5, left, y != 3)
    backward(3)
    for half, cut in pieces:
        take_piece(6, 3 + 4 * first, half, cut)
        send_piece(7, half, cut, right, y != 0)
    send_part(3, right)
    backward(1)
    for half, cut in pieces:
        take_piece(2, 1 + 4 * last, half, cut)
        send_piece(5, half, cut, left, y == 3)
    send_part(1, left)
    backward(8)
    for half, cut in pieces:
        take_piece(7, 4 + 4 * first, half, cut)
        take_piece(5, 8, half, cut, y == 3)
        send_piece(8, half, cut, down)
    backward(4)
    backward(0)

    for h in range(heads):
        cols = pl.ds(h * width, width)
        o_ref[:, cols] = outt_s[h].T
        dq_ref[:, cols] = (dqt_s[h] * (scale * flag)).astype(BF16).T

    for half, cut in pieces:
        take_piece(5, 4, half, cut, y != 3)
        take_piece(3, 4 * first, half, cut)
        take_piece(1, 4, half, cut, y == 3)
        take_piece(8, 4, half, cut)
        send_piece(4, half, cut, down)
    for half, cut in pieces:
        take_piece(1, 0, half, cut, y != 3)
        take_piece(4, 0, half, cut)
    dk_ref[...] = acc[0, 0]
    dv_ref[...] = acc[0, 1]

    for half, cut in pieces:
        for send in range(8):
            block(0, 0, send, half, cut, left).wait_send()
        for slot in range(1, SLOTS):
            part(slot, half, cut, left).wait_send()


def write_out(*refs):
    count = len(refs) // 2
    sems = refs[-1]
    copies = [pltpu.make_async_copy(refs[k], refs[count + k], sems.at[k]) for k in range(count)]
    for copy in copies:
        copy.start()
    for copy in copies:
        copy.wait()


def solution(mesh):
    servers = mesh.shape["server"]
    tiles = servers * mesh.shape["owner"]

    def on_device(queries, key_vectors, value_vectors, out_grad, segments, phase_label):
        tok, width = key_vectors.shape
        heads = queries.shape[1] // width
        seg_rows = segments.reshape(-1, 128)
        vmem = pl.BlockSpec(memory_space=pltpu.VMEM)
        anywhere = pl.BlockSpec(memory_space=pl.ANY)
        results = pl.pallas_call(
            functools.partial(fused, heads, 1.0 / math.sqrt(width), servers, tiles),
            out_shape=(
                pltpu.VMEM((tok, heads * width), BF16),
                pltpu.VMEM((tok, heads * width), BF16),
                pltpu.VMEM((tok, width), F32),
                pltpu.VMEM((tok, width), F32),
            ),
            in_specs=[anywhere] * 5 + [pl.BlockSpec(memory_space=pltpu.SMEM)],
            out_specs=(vmem, vmem, vmem, vmem),
            scratch_shapes=[
                pltpu.VMEM((heads, tok, width), BF16),
                pltpu.VMEM((heads, tok, width), BF16),
                pltpu.VMEM((heads, width, tok), BF16),
                pltpu.VMEM((heads, width, tok), BF16),
                pltpu.VMEM((SLOTS, 2, tok, width), BF16),
                pltpu.VMEM((SLOTS, 2, width, tok), BF16),
                pltpu.VMEM((tiles * tok // 128, 128), jnp.int32),
                pltpu.VMEM((SLOTS, heads, tok, tok), F32),
                pltpu.VMEM((SLOTS, heads, tok, tok), F32),
                pltpu.VMEM((tok, tok), F32),
                pltpu.VMEM((heads, 1, tok), F32),
                pltpu.VMEM((heads, 1, tok), F32),
                pltpu.VMEM((heads, 1, tok), F32),
                pltpu.VMEM((heads, width, tok), F32),
                pltpu.VMEM((heads, width, tok), BF16),
                pltpu.VMEM((heads, width, tok), F32),
                pltpu.VMEM((SLOTS, 2, tok, width), F32),
                pltpu.VMEM((SLOTS, 2, tok, width), BF16),
                pltpu.VMEM((SLOTS, 2, tok, width), BF16),
                pltpu.SemaphoreType.DMA((3 + 2 * heads,)),
                pltpu.SemaphoreType.DMA((8, 2, CUTS)),
                pltpu.SemaphoreType.DMA((SLOTS, 2, CUTS)),
                pltpu.SemaphoreType.DMA((SLOTS, 2, CUTS)),
                pltpu.SemaphoreType.DMA((SLOTS, 2, CUTS)),
            ],
            compiler_params=pltpu.CompilerParams(
                collective_id=0, has_side_effects=True, vmem_limit_bytes=54 * 1024 * 1024
            ),
        )(queries, key_vectors, value_vectors, out_grad, seg_rows, phase_label)
        return pl.pallas_call(
            write_out,
            out_shape=[jax.ShapeDtypeStruct(r.shape, r.dtype) for r in results],
            in_specs=[vmem] * len(results),
            out_specs=[anywhere] * len(results),
            scratch_shapes=[pltpu.SemaphoreType.DMA((len(results),))],
            compiler_params=pltpu.CompilerParams(vmem_limit_bytes=1024 * 1024),
        )(*results)

    tokens = P(("owner", "server"), None)
    return jax.shard_map(
        on_device,
        mesh=mesh,
        in_specs=(tokens, tokens, tokens, tokens, P(), P(("owner", "server"))),
        out_specs=(tokens, tokens, tokens, tokens),
        check_vma=False,
    )
```

```python
import functools
import math

import jax
import jax.numpy as jnp
from jax import lax
from jax.experimental import pallas as pl
from jax.experimental.pallas import tpu as pltpu
from jax.sharding import PartitionSpec as P

MESH = pl.DeviceIdType.MESH
REACH = 8
SLOTS = REACH + 1
ROW = 4
FAR = -1e30
LAG = 3
CUTS = 2
F32 = jnp.float32
BF16 = jnp.bfloat16


def fused(
    heads, scale, servers, tiles,
    q_hbm, k_hbm, v_hbm, do_hbm, seg_hbm, phase_ref,
    o_ref, dq_ref, dk_ref, dv_ref,
    q_s, do_s, qt_s, dot_s, win, win_t, seg_s, s_s, dp_s, bias_s, m_s, l_s, d_s, ot_s, outt_s, dqt_s,
    acc, out_buf, in_buf,
    load_sem, fsend, frecv, bsend, brecv,
):
    tok, width = q_s.shape[1], q_s.shape[2]
    owner = lax.axis_index("owner")
    server = lax.axis_index("server")
    tile = owner * servers + server
    y = server % ROW
    first, last = (y + 3) // 4, y // 3
    rows_of = [pl.ds(k * (tok // CUTS), tok // CUTS) for k in range(CUTS)]
    pieces = [(half, cut) for half in range(2) for cut in range(CUTS)]

    def at_tile(t):
        t = (t + tiles) % tiles
        return (t // servers, t % servers)

    up, down = at_tile(tile + ROW), at_tile(tile - ROW)
    row_start = server - y
    right = (owner, row_start + (y + 1) % ROW)
    left = (owner, row_start + (y + 3) % ROW)

    loads = [pltpu.make_async_copy(k_hbm, win.at[0, 0], load_sem.at[0]),
             pltpu.make_async_copy(v_hbm, win.at[0, 1], load_sem.at[1]),
             pltpu.make_async_copy(seg_hbm, seg_s, load_sem.at[2])]
    for h in range(heads):
        cols = pl.ds(h * width, width)
        loads.append(pltpu.make_async_copy(q_hbm.at[:, cols], q_s.at[h], load_sem.at[3 + h]))
        loads.append(pltpu.make_async_copy(do_hbm.at[:, cols], do_s.at[h], load_sem.at[3 + heads + h]))
    loads[0].start()
    loads[1].start()

    barrier = pltpu.get_barrier_semaphore()
    for peer in (up, down, left, right):
        pl.semaphore_signal(barrier, inc=1, device_id=peer, device_id_type=MESH)
    for copy in loads[2:]:
        copy.start()
    pl.semaphore_wait(barrier, 4)

    def block(src, dst, send, half, cut, peer):
        return pltpu.make_async_remote_copy(
            src_ref=win.at[src, half, rows_of[cut]], dst_ref=win.at[dst, half, rows_of[cut]],
            send_sem=fsend.at[send, half, cut], recv_sem=frecv.at[dst, half, cut],
            device_id=peer, device_id_type=MESH)

    def pass_on(slot, *moves, halves=(0, 1), between=()):
        between = list(between)
        for half, cut in pieces:
            if half not in halves:
                continue
            if slot:
                block(slot, slot, 0, half, cut, left).wait_recv()
            elif cut == 0:
                loads[half].wait()
            for when, dst, send, peer in moves:
                if when is None:
                    block(slot, dst, send, half, cut, peer).start()
                else:
                    @pl.when(when)
                    def _():
                        block(slot, dst, send, half, cut, peer).start()
            if between:
                forward(between.pop(0))

    pass_on(0, (None, 4, 0, up), (y != 3, 1, 1, right), (y == 0, 3, 2, left))

    for copy in loads[2:]:
        copy.wait()
    for h in range(heads):
        qt_s[h] = q_s[h].T
        dot_s[h] = do_s[h].T

    log2e = 1.4426950408889634
    seg_rows = tok // 128

    def seg_row(t):
        parts = [seg_s[pl.ds(t * seg_rows + k, 1), :] for k in range(seg_rows)]
        return jnp.concatenate(parts, axis=1)

    q_seg = seg_row(tile).astype(F32)

    def eight_rows(x, op):
        total = x[0:8]
        for k in range(1, x.shape[0] // 8):
            total = op(total, x[k * 8:(k + 1) * 8])
        return total

    tops = {}

    def forward(slot):
        see_keys(slot)
        use(slot)

    def see_keys(slot):
        owner_tile = tile - slot
        k_seg = seg_row((owner_tile + tiles) % tiles)
        k_seg = jnp.where(owner_tile >= 0, k_seg, -1)
        k_col = jnp.broadcast_to(k_seg.astype(F32), (128, tok)).T
        k_col = jnp.concatenate([k_col] * (tok // 128), axis=1)
        seen = k_col == q_seg
        if slot == 0:
            key_at = lax.broadcasted_iota(jnp.int32, (tok, tok), 0)
            query_at = lax.broadcasted_iota(jnp.int32, (tok, tok), 1)
            seen = seen & (key_at <= query_at)
        bias_s[...] = jnp.where(seen, 0.0, FAR)
        win_t[slot, 0] = win[slot, 0].T

    def score(slot, h):
        s = jnp.dot(win[slot, 0], qt_s[h], preferred_element_type=F32)
        s = s * (scale * log2e) + bias_s[...]
        s_s[slot, h] = s
        tops[slot, h] = jnp.max(eight_rows(s, jnp.maximum), axis=0, keepdims=True)

    def use(slot):
        win_t[slot, 1] = win[slot, 1].T
        scored = (slot, 0) in tops

        def scores(h):
            if not scored:
                score(slot, h)
            dp_s[slot, h] = jnp.dot(win[slot, 1], dot_s[h], preferred_element_type=F32)

        def weigh(h, top):
            if slot:
                old = m_s[h]
                top = jnp.maximum(old, top)
                shrink = jnp.exp2(old - top)
            p = jnp.exp2(s_s[slot, h] - top)
            total = jnp.sum(eight_rows(p, jnp.add), axis=0, keepdims=True)
            out_t = jnp.dot(win_t[slot, 1], p.astype(BF16), preferred_element_type=F32)
            m_s[h] = top
            l_s[h] = l_s[h] * shrink + total if slot else total
            ot_s[h] = ot_s[h] * shrink + out_t if slot else out_t

        for h in range(heads + LAG):
            if h < heads:
                scores(h)
            if h >= LAG:
                weigh(h - LAG, tops[slot, h - LAG])

    forward(0)
    pass_on(4, (None, 8, 3, up), (y != 0, 3, 2, left), (y == 0, 7, 5, left), (y == 3, 1, 1, right), (y != 3, 5, 4, right))
    pass_on(1, (y != 3, 2, 6, right))
    forward(4)
    pass_on(8, (y != 0, 7, 5, left), (y == 3, 5, 4, right))
    pass_on(3, (y == 0, 6, 7, left))
    forward(1)
    pass_on(5, (y == 3, 2, 6, right))
    pass_on(7, (y != 0, 6, 7, left), between=(3, 8, 5))
    forward(7)
    pass_on(2)
    forward(2)
    pass_on(6, halves=(0,))
    see_keys(6)
    for h in range(heads):
        score(6, h)
    pass_on(6, halves=(1,))
    use(6)

    for h in range(heads):
        total = l_s[h]
        out_t = (ot_s[h] * (1.0 / total)).astype(BF16)
        outt_s[h] = out_t
        d_s[h] = jnp.sum(eight_rows(dot_s[h].astype(F32) * out_t.astype(F32), jnp.add), axis=0, keepdims=True)
        m_s[h] = m_s[h] + jnp.log2(total)

    flag = phase_ref[0].astype(F32)

    def backward(slot, first_slot=False, keys=True, values=True):
        dk = dv = None
        for h in range(heads):
            p = jnp.exp2(s_s[slot, h] - m_s[h])
            if keys:
                ds = (p * (dp_s[slot, h] - d_s[h])).astype(BF16)
                dq = jnp.dot(win_t[slot, 0], ds, preferred_element_type=F32)
                dqt_s[h] = dq if first_slot else dqt_s[h] + dq
                dk_h = jnp.dot(ds, q_s[h], preferred_element_type=F32)
                dk = dk_h if h == 0 else dk + dk_h
            if values:
                dv_h = jnp.dot(p.astype(BF16), do_s[h], preferred_element_type=F32)
                dv = dv_h if h == 0 else dv + dv_h
        if keys:
            dk = dk * (scale * flag)
            acc[slot, 0] = acc[slot, 0] + dk if slot == 4 else dk
        if values:
            dv = dv * flag
            acc[slot, 1] = acc[slot, 1] + dv if slot == 4 else dv

    back = [(half, cut) for half in (1, 0) for cut in range(CUTS)]

    def part(slot, half, cut, peer):
        return pltpu.make_async_remote_copy(
            src_ref=out_buf.at[slot, half, rows_of[cut]], dst_ref=in_buf.at[slot, half, rows_of[cut]],
            send_sem=bsend.at[slot, half, cut], recv_sem=brecv.at[slot, half, cut],
            device_id=peer, device_id_type=MESH)

    def send_piece(slot, half, cut, peer, when=None):
        def send():
            out_buf[slot, half, rows_of[cut]] = acc[slot, half, rows_of[cut]].astype(BF16)
            part(slot, half, cut, peer).start()

        send() if when is None else pl.when(when)(send)

    def send_part(slot, peer, when=None, halves=(1, 0)):
        for half, cut in back:
            if half in halves:
                send_piece(slot, half, cut, peer, when)

    def take_piece(slot, into, half, cut, when=None):
        def take():
            part(slot, half, cut, left).wait_recv()
            rows = rows_of[cut]
            acc[into, half, rows] = acc[into, half, rows] + in_buf[slot, half, rows].astype(F32)

        take() if when is None else pl.when(when)(take)

    acc[4] = jnp.zeros(acc.shape[1:], F32)
    backward(6, keys=False)
    send_part(6, right, halves=(1,))
    backward(6, True, values=False)
    send_part(6, right, halves=(0,))
    backward(2)
    send_part(2, left)
    backward(7)
    send_part(7, right, y == 0)
    backward(5)
    send_part(5, left, y != 3)
    backward(3)
    for half, cut in back:
        take_piece(6, 3 + 4 * first, half, cut)
        send_piece(7, half, cut, right, y != 0)
    send_part(3, right)
    backward(1)
    for half, cut in back:
        take_piece(2, 1 + 4 * last, half, cut)
        send_piece(5, half, cut, left, y == 3)
    send_part(1, left)
    backward(8)
    for half, cut in back:
        take_piece(7, 4 + 4 * first, half, cut)
        take_piece(5, 8, half, cut, y == 3)
        send_piece(8, half, cut, down)
    backward(4)
    backward(0)

    for h in range(heads):
        cols = pl.ds(h * width, width)
        o_ref[:, cols] = outt_s[h].T
        dq_ref[:, cols] = (dqt_s[h] * (scale * flag)).astype(BF16).T

    for half, cut in back:
        for send in range(8):
            block(0, 0, send, half, cut, left).wait_send()
        for slot in (2, 5, 6, 7):
            part(slot, half, cut, left).wait_send()

    for half, cut in back:
        take_piece(5, 4, half, cut, y != 3)
        take_piece(3, 4 * first, half, cut)
        take_piece(1, 4, half, cut, y == 3)
        take_piece(8, 4, half, cut)
        send_piece(4, half, cut, down)
    for half, cut in back:
        take_piece(1, 0, half, cut, y != 3)
        for slot in (1, 3, 8):
            part(slot, half, cut, left).wait_send()
    for half, cut in back:
        part(4, half, cut, left).wait_recv()
        rows = rows_of[cut]
        grad_ref = (dk_ref, dv_ref)[half]
        grad_ref[rows, :] = acc[0, half, rows] + in_buf[4, half, rows].astype(F32)
    for half, cut in back:
        part(4, half, cut, left).wait_send()


def write_out(*refs):
    count = len(refs) // 2
    sems = refs[-1]
    copies = [pltpu.make_async_copy(refs[k], refs[count + k], sems.at[k]) for k in range(count)]
    for copy in copies:
        copy.start()
    for copy in copies:
        copy.wait()


def solution(mesh):
    servers = mesh.shape["server"]
    tiles = servers * mesh.shape["owner"]

    def on_device(queries, key_vectors, value_vectors, out_grad, segments, phase_label):
        tok, width = key_vectors.shape
        heads = queries.shape[1] // width
        seg_rows = segments.reshape(-1, 128)
        vmem = pl.BlockSpec(memory_space=pltpu.VMEM)
        anywhere = pl.BlockSpec(memory_space=pl.ANY)
        results = pl.pallas_call(
            functools.partial(fused, heads, 1.0 / math.sqrt(width), servers, tiles),
            out_shape=(
                pltpu.VMEM((tok, heads * width), BF16),
                pltpu.VMEM((tok, heads * width), BF16),
                pltpu.VMEM((tok, width), F32),
                pltpu.VMEM((tok, width), F32),
            ),
            in_specs=[anywhere] * 5 + [pl.BlockSpec(memory_space=pltpu.SMEM)],
            out_specs=(vmem, vmem, vmem, vmem),
            scratch_shapes=[
                pltpu.VMEM((heads, tok, width), BF16),
                pltpu.VMEM((heads, tok, width), BF16),
                pltpu.VMEM((heads, width, tok), BF16),
                pltpu.VMEM((heads, width, tok), BF16),
                pltpu.VMEM((SLOTS, 2, tok, width), BF16),
                pltpu.VMEM((SLOTS, 2, width, tok), BF16),
                pltpu.VMEM((tiles * tok // 128, 128), jnp.int32),
                pltpu.VMEM((SLOTS, heads, tok, tok), F32),
                pltpu.VMEM((SLOTS, heads, tok, tok), F32),
                pltpu.VMEM((tok, tok), F32),
                pltpu.VMEM((heads, 1, tok), F32),
                pltpu.VMEM((heads, 1, tok), F32),
                pltpu.VMEM((heads, 1, tok), F32),
                pltpu.VMEM((heads, width, tok), F32),
                pltpu.VMEM((heads, width, tok), BF16),
                pltpu.VMEM((heads, width, tok), F32),
                pltpu.VMEM((SLOTS, 2, tok, width), F32),
                pltpu.VMEM((SLOTS, 2, tok, width), BF16),
                pltpu.VMEM((SLOTS, 2, tok, width), BF16),
                pltpu.SemaphoreType.DMA((3 + 2 * heads,)),
                pltpu.SemaphoreType.DMA((8, 2, CUTS)),
                pltpu.SemaphoreType.DMA((SLOTS, 2, CUTS)),
                pltpu.SemaphoreType.DMA((SLOTS, 2, CUTS)),
                pltpu.SemaphoreType.DMA((SLOTS, 2, CUTS)),
            ],
            compiler_params=pltpu.CompilerParams(
                collective_id=0, has_side_effects=True, vmem_limit_bytes=54 * 1024 * 1024
            ),
        )(queries, key_vectors, value_vectors, out_grad, seg_rows, phase_label)
        return pl.pallas_call(
            write_out,
            out_shape=[jax.ShapeDtypeStruct(r.shape, r.dtype) for r in results],
            in_specs=[vmem] * len(results),
            out_specs=[anywhere] * len(results),
            scratch_shapes=[pltpu.SemaphoreType.DMA((len(results),))],
            compiler_params=pltpu.CompilerParams(vmem_limit_bytes=1024 * 1024),
        )(*results)

    tokens = P(("owner", "server"), None)
    return jax.shard_map(
        on_device,
        mesh=mesh,
        in_specs=(tokens, tokens, tokens, tokens, P(), P(("owner", "server"))),
        out_specs=(tokens, tokens, tokens, tokens),
        check_vma=False,
    )
```

```python
import functools
import math

import jax
import jax.numpy as jnp
from jax import lax
from jax.experimental import pallas as pl
from jax.experimental.pallas import tpu as pltpu
from jax.sharding import PartitionSpec as P

MESH = pl.DeviceIdType.MESH
REACH = 8
SLOTS = REACH + 1
ROW = 4
FAR = -1e30
LAG = 3
CUTS = 2
F32 = jnp.float32
BF16 = jnp.bfloat16


def fused(
    heads, scale, servers, tiles,
    q_hbm, k_hbm, v_hbm, do_hbm, seg_hbm, phase_ref,
    o_ref, dq_ref, dk_ref, dv_ref,
    q_s, do_s, qt_s, dot_s, win, win_t, seg_s, s_s, dp_s, bias_s, m_s, l_s, d_s, ot_s, outt_s, dqt_s,
    acc, out_buf, in_buf,
    load_sem, fsend, frecv, bsend, brecv,
):
    tok, width = q_s.shape[1], q_s.shape[2]
    owner = lax.axis_index("owner")
    server = lax.axis_index("server")
    tile = owner * servers + server
    y = server % ROW
    first, last = (y + 3) // 4, y // 3
    rows_of = [pl.ds(k * (tok // CUTS), tok // CUTS) for k in range(CUTS)]
    pieces = [(half, cut) for half in range(2) for cut in range(CUTS)]

    def at_tile(t):
        t = (t + tiles) % tiles
        return (t // servers, t % servers)

    up, down = at_tile(tile + ROW), at_tile(tile - ROW)
    row_start = server - y
    right = (owner, row_start + (y + 1) % ROW)
    left = (owner, row_start + (y + 3) % ROW)

    loads = [pltpu.make_async_copy(k_hbm, win.at[0, 0], load_sem.at[0]),
             pltpu.make_async_copy(v_hbm, win.at[0, 1], load_sem.at[1]),
             pltpu.make_async_copy(seg_hbm, seg_s, load_sem.at[2])]
    for h in range(heads):
        cols = pl.ds(h * width, width)
        loads.append(pltpu.make_async_copy(q_hbm.at[:, cols], q_s.at[h], load_sem.at[3 + h]))
        loads.append(pltpu.make_async_copy(do_hbm.at[:, cols], do_s.at[h], load_sem.at[3 + heads + h]))
    loads[0].start()
    loads[1].start()

    barrier = pltpu.get_barrier_semaphore()
    for peer in (up, down, left, right):
        pl.semaphore_signal(barrier, inc=1, device_id=peer, device_id_type=MESH)
    for copy in loads[2:]:
        copy.start()
    pl.semaphore_wait(barrier, 4)

    def block(src, dst, send, half, cut, peer):
        return pltpu.make_async_remote_copy(
            src_ref=win.at[src, half, rows_of[cut]], dst_ref=win.at[dst, half, rows_of[cut]],
            send_sem=fsend.at[send, half, cut], recv_sem=frecv.at[dst, half, cut],
            device_id=peer, device_id_type=MESH)

    def pass_on(slot, *moves, between=()):
        between = list(between)
        for half, cut in pieces:
            if slot:
                block(slot, slot, 0, half, cut, left).wait_recv()
            elif cut == 0:
                loads[half].wait()
            for when, dst, send, peer in moves:
                if when is None:
                    block(slot, dst, send, half, cut, peer).start()
                else:
                    @pl.when(when)
                    def _():
                        block(slot, dst, send, half, cut, peer).start()
            if between:
                forward(between.pop(0))

    pass_on(0, (None, 4, 0, up), (y != 3, 1, 1, right), (y == 0, 3, 2, left))

    for copy in loads[2:]:
        copy.wait()
    for h in range(heads):
        qt_s[h] = q_s[h].T
        dot_s[h] = do_s[h].T

    log2e = 1.4426950408889634
    seg_rows = tok // 128

    def seg_row(t):
        parts = [seg_s[pl.ds(t * seg_rows + k, 1), :] for k in range(seg_rows)]
        return jnp.concatenate(parts, axis=1)

    q_seg = seg_row(tile).astype(F32)

    def eight_rows(x, op):
        total = x[0:8]
        for k in range(1, x.shape[0] // 8):
            total = op(total, x[k * 8:(k + 1) * 8])
        return total

    def forward(slot):
        owner_tile = tile - slot
        k_seg = seg_row((owner_tile + tiles) % tiles)
        k_seg = jnp.where(owner_tile >= 0, k_seg, -1)
        k_col = jnp.broadcast_to(k_seg.astype(F32), (128, tok)).T
        k_col = jnp.concatenate([k_col] * (tok // 128), axis=1)
        seen = k_col == q_seg
        if slot == 0:
            key_at = lax.broadcasted_iota(jnp.int32, (tok, tok), 0)
            query_at = lax.broadcasted_iota(jnp.int32, (tok, tok), 1)
            seen = seen & (key_at <= query_at)
        bias_s[...] = jnp.where(seen, 0.0, FAR)
        win_t[slot, 0] = win[slot, 0].T
        win_t[slot, 1] = win[slot, 1].T

        def scores(h):
            s = jnp.dot(win[slot, 0], qt_s[h], preferred_element_type=F32)
            s = s * (scale * log2e) + bias_s[...]
            s_s[slot, h] = s
            dp_s[slot, h] = jnp.dot(win[slot, 1], dot_s[h], preferred_element_type=F32)
            return jnp.max(eight_rows(s, jnp.maximum), axis=0, keepdims=True)

        def weigh(h, top):
            if slot:
                old = m_s[h]
                top = jnp.maximum(old, top)
                shrink = jnp.exp2(old - top)
            p = jnp.exp2(s_s[slot, h] - top)
            total = jnp.sum(eight_rows(p, jnp.add), axis=0, keepdims=True)
            out_t = jnp.dot(win_t[slot, 1], p.astype(BF16), preferred_element_type=F32)
            m_s[h] = top
            l_s[h] = l_s[h] * shrink + total if slot else total
            ot_s[h] = ot_s[h] * shrink + out_t if slot else out_t

        tops = []
        for h in range(heads + LAG):
            if h < heads:
                tops.append(scores(h))
            if h >= LAG:
                weigh(h - LAG, tops[h - LAG])

    forward(0)
    pass_on(4, (None, 8, 3, up), (y != 0, 3, 2, left), (y == 0, 7, 5, left), (y == 3, 1, 1, right), (y != 3, 5, 4, right))
    pass_on(1, (y != 3, 2, 6, right))
    forward(4)
    pass_on(8, (y != 0, 7, 5, left), (y == 3, 5, 4, right))
    pass_on(3, (y == 0, 6, 7, left))
    forward(1)
    pass_on(5, (y == 3, 2, 6, right))
    pass_on(7, (y != 0, 6, 7, left), between=(3, 8, 5))
    forward(7)
    pass_on(2)
    forward(2)
    pass_on(6)
    forward(6)

    for h in range(heads):
        total = l_s[h]
        out_t = (ot_s[h] * (1.0 / total)).astype(BF16)
        outt_s[h] = out_t
        d_s[h] = jnp.sum(eight_rows(dot_s[h].astype(F32) * out_t.astype(F32), jnp.add), axis=0, keepdims=True)
        m_s[h] = m_s[h] + jnp.log2(total)

    flag = phase_ref[0].astype(F32)

    def backward(slot, first_slot=False):
        dk = dv = None
        for h in range(heads):
            p = jnp.exp2(s_s[slot, h] - m_s[h])
            ds = (p * (dp_s[slot, h] - d_s[h])).astype(BF16)
            dq = jnp.dot(win_t[slot, 0], ds, preferred_element_type=F32)
            dqt_s[h] = dq if first_slot else dqt_s[h] + dq
            dk_h = jnp.dot(ds, q_s[h], preferred_element_type=F32)
            dv_h = jnp.dot(p.astype(BF16), do_s[h], preferred_element_type=F32)
            dk = dk_h if h == 0 else dk + dk_h
            dv = dv_h if h == 0 else dv + dv_h
        dk, dv = dk * (scale * flag), dv * flag
        acc[slot, 0] = acc[slot, 0] + dk if slot == 4 else dk
        acc[slot, 1] = acc[slot, 1] + dv if slot == 4 else dv

    def part(slot, half, cut, peer):
        return pltpu.make_async_remote_copy(
            src_ref=out_buf.at[slot, half, rows_of[cut]], dst_ref=in_buf.at[slot, half, rows_of[cut]],
            send_sem=bsend.at[slot, half, cut], recv_sem=brecv.at[slot, half, cut],
            device_id=peer, device_id_type=MESH)

    def send_piece(slot, half, cut, peer, when=None):
        def send():
            out_buf[slot, half, rows_of[cut]] = acc[slot, half, rows_of[cut]].astype(BF16)
            part(slot, half, cut, peer).start()

        send() if when is None else pl.when(when)(send)

    def send_part(slot, peer, when=None):
        for half, cut in pieces:
            send_piece(slot, half, cut, peer, when)

    def take_piece(slot, into, half, cut, when=None):
        def take():
            part(slot, half, cut, left).wait_recv()
            rows = rows_of[cut]
            acc[into, half, rows] = acc[into, half, rows] + in_buf[slot, half, rows].astype(F32)

        take() if when is None else pl.when(when)(take)

    acc[4] = jnp.zeros(acc.shape[1:], F32)
    backward(6, True)
    send_part(6, right)
    backward(2)
    send_part(2, left)
    backward(7)
    send_part(7, right, y == 0)
    backward(5)
    send_part(5, left, y != 3)
    backward(3)
    for half, cut in pieces:
        take_piece(6, 3 + 4 * first, half, cut)
        send_piece(7, half, cut, right, y != 0)
    send_part(3, right)
    backward(1)
    for half, cut in pieces:
        take_piece(2, 1 + 4 * last, half, cut)
        send_piece(5, half, cut, left, y == 3)
    send_part(1, left)
    backward(8)
    for half, cut in pieces:
        take_piece(7, 4 + 4 * first, half, cut)
        take_piece(5, 8, half, cut, y == 3)
        send_piece(8, half, cut, down)
    backward(4)
    backward(0)

    for h in range(heads):
        cols = pl.ds(h * width, width)
        o_ref[:, cols] = outt_s[h].T
        dq_ref[:, cols] = (dqt_s[h] * (scale * flag)).astype(BF16).T

    for half, cut in pieces:
        for send in range(8):
            block(0, 0, send, half, cut, left).wait_send()
        for slot in (2, 5, 6, 7):
            part(slot, half, cut, left).wait_send()

    for half, cut in pieces:
        take_piece(5, 4, half, cut, y != 3)
        take_piece(3, 4 * first, half, cut)
        take_piece(1, 4, half, cut, y == 3)
        take_piece(8, 4, half, cut)
        send_piece(4, half, cut, down)
    for half, cut in pieces:
        take_piece(1, 0, half, cut, y != 3)
        for slot in (1, 3, 8):
            part(slot, half, cut, left).wait_send()
    for half, cut in pieces:
        part(4, half, cut, left).wait_recv()
        rows = rows_of[cut]
        grad_ref = (dk_ref, dv_ref)[half]
        grad_ref[rows, :] = acc[0, half, rows] + in_buf[4, half, rows].astype(F32)
    for half, cut in pieces:
        part(4, half, cut, left).wait_send()


def write_out(*refs):
    count = len(refs) // 2
    sems = refs[-1]
    copies = [pltpu.make_async_copy(refs[k], refs[count + k], sems.at[k]) for k in range(count)]
    for copy in copies:
        copy.start()
    for copy in copies:
        copy.wait()


def solution(mesh):
    servers = mesh.shape["server"]
    tiles = servers * mesh.shape["owner"]

    def on_device(queries, key_vectors, value_vectors, out_grad, segments, phase_label):
        tok, width = key_vectors.shape
        heads = queries.shape[1] // width
        seg_rows = segments.reshape(-1, 128)
        vmem = pl.BlockSpec(memory_space=pltpu.VMEM)
        anywhere = pl.BlockSpec(memory_space=pl.ANY)
        results = pl.pallas_call(
            functools.partial(fused, heads, 1.0 / math.sqrt(width), servers, tiles),
            out_shape=(
                pltpu.VMEM((tok, heads * width), BF16),
                pltpu.VMEM((tok, heads * width), BF16),
                pltpu.VMEM((tok, width), F32),
                pltpu.VMEM((tok, width), F32),
            ),
            in_specs=[anywhere] * 5 + [pl.BlockSpec(memory_space=pltpu.SMEM)],
            out_specs=(vmem, vmem, vmem, vmem),
            scratch_shapes=[
                pltpu.VMEM((heads, tok, width), BF16),
                pltpu.VMEM((heads, tok, width), BF16),
                pltpu.VMEM((heads, width, tok), BF16),
                pltpu.VMEM((heads, width, tok), BF16),
                pltpu.VMEM((SLOTS, 2, tok, width), BF16),
                pltpu.VMEM((SLOTS, 2, width, tok), BF16),
                pltpu.VMEM((tiles * tok // 128, 128), jnp.int32),
                pltpu.VMEM((SLOTS, heads, tok, tok), F32),
                pltpu.VMEM((SLOTS, heads, tok, tok), F32),
                pltpu.VMEM((tok, tok), F32),
                pltpu.VMEM((heads, 1, tok), F32),
                pltpu.VMEM((heads, 1, tok), F32),
                pltpu.VMEM((heads, 1, tok), F32),
                pltpu.VMEM((heads, width, tok), F32),
                pltpu.VMEM((heads, width, tok), BF16),
                pltpu.VMEM((heads, width, tok), F32),
                pltpu.VMEM((SLOTS, 2, tok, width), F32),
                pltpu.VMEM((SLOTS, 2, tok, width), BF16),
                pltpu.VMEM((SLOTS, 2, tok, width), BF16),
                pltpu.SemaphoreType.DMA((3 + 2 * heads,)),
                pltpu.SemaphoreType.DMA((8, 2, CUTS)),
                pltpu.SemaphoreType.DMA((SLOTS, 2, CUTS)),
                pltpu.SemaphoreType.DMA((SLOTS, 2, CUTS)),
                pltpu.SemaphoreType.DMA((SLOTS, 2, CUTS)),
            ],
            compiler_params=pltpu.CompilerParams(
                collective_id=0, has_side_effects=True, vmem_limit_bytes=54 * 1024 * 1024
            ),
        )(queries, key_vectors, value_vectors, out_grad, seg_rows, phase_label)
        return pl.pallas_call(
            write_out,
            out_shape=[jax.ShapeDtypeStruct(r.shape, r.dtype) for r in results],
            in_specs=[vmem] * len(results),
            out_specs=[anywhere] * len(results),
            scratch_shapes=[pltpu.SemaphoreType.DMA((len(results),))],
            compiler_params=pltpu.CompilerParams(vmem_limit_bytes=1024 * 1024),
        )(*results)

    tokens = P(("owner", "server"), None)
    return jax.shard_map(
        on_device,
        mesh=mesh,
        in_specs=(tokens, tokens, tokens, tokens, P(), P(("owner", "server"))),
        out_specs=(tokens, tokens, tokens, tokens),
        check_vma=False,
    )
```
